32 devices in a mesh: row: 4 (over x, core), col: 8 (over z, y).
Axes of the slice: x: 2, y: 2, z: 4, core: 2. Of those that a mesh axis runs over, the one named last changes fastest.
Arguments:
- diag_block: float32 [512, 512], P(None, 'col'), may hold values from -0.2 to 2, as said below
- panel_below: float32 [2048, 512], P('col', 'row'), may hold values from -0.26516503 to 0.26516503
- trail_inverse: float32 [2048, 2048], P('row', 'col'), may hold values from -0.125 to 0.125
Outputs:
- inverse_panel: float32 [2048, 512], P('row', 'col')
- product_panel: float32 [2048, 512], P('col', 'row')
The draws below stay inside these ranges and needn't reach their ends.
Inputs may be any that keep to these rules, and one draw needn't show every extreme that they name: diag_block is lower triangular with diagonal entries between 1 and 2 and off-diagonal entries of magnitude at most 0.2.
All inputs are finite; a program needn't handle non-finite values.
Results may differ from the reference program's by a relative error of at most 0.000094.
Values sent between devices are 32-bit elements; how exact they have to be, the bound alone decides.
A program may use at most 64 MiB of HBM per device.

```python
import jax
import jax.numpy as jnp
from jax import lax

BLOCK = 512
M = 2048
CYC = 256
N_ROW = 4
N_COL = 8


def draw_diag_block(key, part):
    first, second = jax.random.split(jax.random.fold_in(key, 11))
    lower = jnp.clip(jax.random.normal(first, (BLOCK, BLOCK), jnp.float32) * (0.5 / BLOCK ** 0.5), -0.2, 0.2)
    diagonal = jax.random.uniform(second, (BLOCK,), jnp.float32, 1.0, 2.0)
    return jnp.tril(lower, -1) + jnp.diag(diagonal)


def shard_levels(stream_key, dims, shards, least, top_value):
    def one(dim, shards_of):
        heights = jax.random.uniform(jax.random.fold_in(jax.random.fold_in(stream_key, 6), dim), (shards_of,), jnp.float32, least / len(shards), top_value / len(shards))
        return jnp.repeat(jnp.exp(heights), dims[dim] // shards_of).reshape((-1,) + (1,) * (len(dims) - dim - 1))

    gain = one(*shards[0])
    for cut in shards[1:]:
        gain = gain * one(*cut)
    return gain


def scatter_about(key, extent, deviation, reach, cuts=(), kind=jnp.bfloat16):
    gain = shard_levels(key, extent, cuts, -0.22, 0.18) if cuts else 1.0
    drawn = jax.random.normal(key, extent, jnp.float32) * deviation * gain
    return jnp.minimum(jnp.maximum(drawn, -reach), reach).astype(kind)


def setup_inputs(seed: int = 0) -> dict:
    key_of = jax.random.split(jax.random.key(seed), 4)
    diag_block = draw_diag_block(jax.random.fold_in(key_of[3], 71), 0)
    panel_below = scatter_about(key_of[1], (M, BLOCK), (BLOCK ** -0.5), 0.26516503, ((0, 8), (1, 4)), jnp.float32)
    trail_inverse = scatter_about(key_of[2], (M, M), M ** -0.5, 0.125, ((0, 4), (1, 8)), jnp.float32)
    return dict(diag_block=diag_block, panel_below=panel_below, trail_inverse=trail_inverse)


def storage_map(count, parts):
    position = jnp.arange(M, dtype=jnp.int32)
    per_part = M // parts
    owner = position // per_part
    local = position % per_part
    return (local // CYC * parts + owner) * CYC + local % CYC

def reference(diag_block, panel_below, trail_inverse):
    high = lax.Precision.HIGHEST
    eye_block = jnp.eye(BLOCK, dtype=jnp.float32)
    inverse_block = jax.scipy.linalg.solve_triangular(diag_block, eye_block, lower=True)
    scaled = jnp.dot(panel_below.astype(jnp.float32), inverse_block.astype(jnp.float32), precision=high, preferred_element_type=jnp.float32)
    rowmap = storage_map(M, N_ROW)
    colmap = storage_map(M, N_COL)
    below = rowmap[:, None] >= colmap[None, :]
    same = rowmap[:, None] == colmap[None, :]
    factor = jnp.where(below, trail_inverse, jnp.float32(0.0)) + jnp.where(same, jnp.float32(1.0), jnp.float32(0.0))
    inverse_panel = -jnp.dot(factor.astype(jnp.float32), scaled.astype(jnp.float32), precision=high, preferred_element_type=jnp.float32)
    product_panel = lax.dot_general(factor.astype(jnp.float32), inverse_panel.astype(jnp.float32), (((0,), (0,)), ((), ())), precision=high, preferred_element_type=jnp.float32)
    return (inverse_panel, product_panel)
```

```python
import functools

import jax
import jax.numpy as jnp
from jax import lax
from jax.experimental import pallas as pl
from jax.experimental.pallas import tpu as pltpu
from jax.sharding import PartitionSpec as P

F32 = jnp.float32
BF16 = jnp.bfloat16
MESH = pl.DeviceIdType.MESH
LANES = 128
SEED = 16


def split(value):
    high = value.astype(BF16)
    return high, (value - high.astype(F32)).astype(BF16)


def dot_split(left, right):
    lh, ll = left
    rh, rl = right
    return (
        jnp.dot(lh, rh, preferred_element_type=F32)
        + jnp.dot(lh, rl, preferred_element_type=F32)
        + jnp.dot(ll, rh, preferred_element_type=F32)
    )


def dot3(left, right):
    return dot_split(split(left), split(right))


def repeat(count, step):
    if count == 1:
        step(0)
    else:
        lax.fori_loop(0, count, lambda i, _: (step(i), 0)[1], 0)


def invert_seed_blocks(m_ref, x_ref, dinv_ref, l_ref, width):
    row = lax.broadcasted_iota(jnp.int32, (LANES, LANES), 0)
    col = lax.broadcasted_iota(jnp.int32, (LANES, LANES), 1)
    eye = row == col
    low = row > col
    eye_f = jnp.where(eye, 1.0, 0.0).astype(F32)
    blocks = width // LANES
    ms, ns, ps = [], [], []
    for b in range(blocks):
        at = slice(b * LANES, (b + 1) * LANES)
        block = l_ref[at, at]
        diagonal = jnp.where(eye, block, 0.0)
        dinv_ref[0:1, at] = 1.0 / jnp.sum(diagonal, axis=0, keepdims=True)
        scale = 1.0 / jnp.sum(diagonal, axis=1, keepdims=True)
        if b:
            m_ref[at, 0 : b * LANES] = l_ref[at, 0 : b * LANES] * scale
        m = jnp.where(low, block * scale, 0.0)
        n = jnp.where(row // SEED == col // SEED, -m, 0.0)
        ms.append(m)
        ns.append(n)
        ps.append(eye_f + n)
    size = 2
    while size < SEED:
        halves = [split(n) for n in ns]
        ns = [dot_split(h, h) for h in halves]
        ps = [p + dot3(p, n) for p, n in zip(ps, ns)]
        size *= 2
    size = SEED
    while size < LANES:
        off = jnp.logical_and((row // size) % 2 == 1, col // size == row // size - 1)
        pairs = [split(p) for p in ps]
        mid = [dot_split(split(jnp.where(off, m, 0.0)), q) for m, q in zip(ms, pairs)]
        ps = [p - dot_split(q, split(t)) for p, q, t in zip(ps, pairs, mid)]
        size *= 2
    x_ref[...] = jnp.zeros_like(x_ref)
    for b in range(blocks):
        at = slice(b * LANES, (b + 1) * LANES)
        x_ref[at, at] = ps[b]


def invert_double(m_ref, x_ref, width):
    size = LANES
    while size < width:
        for p in range(0, width, 2 * size):
            a, b = slice(p, p + size), slice(p + size, p + 2 * size)
            x_ref[b, a] = -dot3(x_ref[b, b], dot3(m_ref[b, a], x_ref[a, a]))
        size *= 2


def kernel(
    R, C, G,
    diag_ref, panel_ref, trail_ref, ip_ref, pp_ref,
    lbuf, pbuf, pfull, whi, wlo, wthi, wtlo, zpart, yrecv, zsend, zrecv,
    lmat, mmat, xmat, dinv, ipfull, ppbuf, ppair, pxsend, pxrecv,
    d1_s, d1_r, d2_s, d2_r, d2f_s, d2f_r, p_s, p_r, pf_s, pf_r,
    y_s, y_r, z_s, z_r, ag_s, ag_r, agy_s, agy_r, f1_s, f1_r, f2_s, f2_r,
):
    r, c = lax.axis_index("row"), lax.axis_index("col")
    X, Z = R // 2, C // G
    x, core = r // 2, r % 2
    z, y = c // G, c % G
    partner = x * 2 + 1 - core
    width = lmat.shape[0]
    share = width // C
    rows, cols = trail_ref.shape
    pwidth = width // R
    chunk = rows // C

    def x_peer(k):
        return lax.rem(x + k, X) * 2 + core

    def x_from(k):
        return lax.rem(x + X - k, X) * 2 + core

    def over(a):
        return a // 2 * 2 + 1 - a % 2

    def z_peer(k):
        return lax.rem(z + k, Z) * G + y

    def z_from(k):
        return lax.rem(z + Z - k, Z) * G + y

    def y_peer(k):
        return z * G + lax.rem(y + k, G)

    def copy(src, dst, s, d, **where):
        return pltpu.make_async_remote_copy(
            src_ref=src, dst_ref=dst, send_sem=s, recv_sem=d,
            device_id=where, device_id_type=MESH,
        )

    barrier = pltpu.get_barrier_semaphore()
    for k in range(1, R):
        pl.semaphore_signal(barrier, inc=1, device_id={"row": lax.rem(r + k, R)}, device_id_type=MESH)
    for k in range(1, C):
        pl.semaphore_signal(barrier, inc=1, device_id={"col": lax.rem(c + k, C)}, device_id_type=MESH)

    packs = LANES // share
    tall = width // packs
    part = tall // R
    for q in range(packs):
        lbuf[r, c, :, q * share : (q + 1) * share] = diag_ref[pl.ds(q * tall + r * part, part), :]
    pl.semaphore_wait(barrier, R + C - 2)

    pending = []

    def go(one):
        one.start()
        pending.append(one)
        return one

    p_far = [go(copy(panel_ref, pbuf.at[r], p_s.at[k], p_r.at[k], row=x_peer(k))) for k in range(1, X)]
    p_near = go(copy(panel_ref, pbuf.at[r], p_s.at[0], p_r.at[0], row=partner))
    d1 = [
        go(copy(lbuf.at[r, c], lbuf.at[r, c], d1_s.at[k], d1_r.at[k], col=lax.rem(c + k, C)))
        for k in range(1, C)
    ]
    pbuf[r] = panel_ref[...]

    cycle = min(512, cols)
    tile = min(512, rows)

    def form(i):
        at = pl.ds(pl.multiple_of(i * tile, tile), tile)
        lr = lax.broadcasted_iota(jnp.int32, (tile, cols), 0) + i * tile
        lc = lax.broadcasted_iota(jnp.int32, (tile, cols), 1)
        gr = (lr // cycle * R + r) * cycle + lr % cycle
        gc = (lc // cycle * C + c) * cycle + lc % cycle
        w = jnp.where(gr >= gc, trail_ref[at, :], 0.0) + jnp.where(gr == gc, 1.0, 0.0).astype(F32)
        hi, lo = split(w)
        whi[at, :] = hi
        wlo[at, :] = lo
        hi, lo = split(w.T)
        wthi[:, at] = hi
        wtlo[:, at] = lo

    repeat(rows // tile, form)

    p_fwd = []
    for k in range(1, X):
        p_far[k - 1].wait_recv()
        src = pbuf.at[x_from(k)]
        p_fwd.append(go(copy(src, src, pf_s.at[k], pf_r.at[k], row=partner)))
    p_near.wait_recv()
    for one in p_fwd:
        one.wait_recv()
    for a in range(R):
        pfull[:, a * pwidth : (a + 1) * pwidth] = pbuf[a]
    pair = split(pfull[...])

    def product(i):
        at = pl.ds(pl.multiple_of(i * tile, tile), tile)
        zpart[at, :] = dot_split((whi[at, :], wlo[at, :]), pair)

    repeat(rows // tile, product)

    def rows_of(owner):
        return pl.ds(pl.multiple_of(owner * chunk, chunk), chunk)

    order = list(range(1, Z)) + [0]
    y_sends = {}
    for k in order:
        for g in range(1, G):
            dst_owner = lax.rem(z + k, Z) * G + lax.rem(y + g, G)
            y_sends[k, g] = go(
                copy(zpart.at[rows_of(dst_owner), :], yrecv.at[g - 1, k], y_s.at[g, k], y_r.at[g, k], col=y_peer(g))
            )

    for one in d1:
        one.wait_recv()
    d2_far = [go(copy(lbuf.at[r], lbuf.at[r], d2_s.at[k], d2_r.at[k], row=x_peer(k))) for k in range(1, X)]
    d2_near = go(copy(lbuf.at[r], lbuf.at[r], d2_s.at[0], d2_r.at[0], row=partner))

    z_sends = []
    d2_fwd = []
    for step, k in enumerate(order):
        total = zpart[rows_of(z_peer(k)), :]
        for g in range(1, G):
            y_sends[k, g].wait_recv()
            total = total + yrecv[g - 1, k]
        zsend[k] = total
        if k:
            z_sends.append(go(copy(zsend.at[k], zrecv.at[k], z_s.at[k], z_r.at[k], col=z_peer(k))))
        if step == Z // 2:
            for j in range(1, X):
                d2_far[j - 1].wait_recv()
                src = lbuf.at[x_from(j)]
                d2_fwd.append(go(copy(src, src, d2f_s.at[j], d2f_r.at[j], row=partner)))

    d2_near.wait_recv()
    for one in d2_fwd:
        one.wait_recv()
    for q in range(packs):
        for a in range(R):
            at = slice(q * tall + a * part, q * tall + (a + 1) * part)
            for b in range(C):
                lmat[at, b * share : (b + 1) * share] = lbuf[a, b, :, q * share : (q + 1) * share]
    invert_seed_blocks(mmat, xmat, dinv, lmat, width)
    invert_double(mmat, xmat, width)

    total = zsend[0]
    for one, k in zip(z_sends, range(1, Z)):
        one.wait_recv()
        total = total + zrecv[k]
    ipfull[c] = -dot3(total, xmat[...]) * dinv[0:1, :]

    mine = ipfull.at[c]
    ag_z = [go(copy(mine, mine, ag_s.at[k], ag_r.at[k], col=z_peer(k))) for k in range(1, Z)]
    ag_y = [go(copy(mine, mine, agy_s.at[g, 0], agy_r.at[g, 0], col=y_peer(g))) for g in range(1, G)]
    for k in range(1, Z):
        ag_z[k - 1].wait_recv()
        src = ipfull.at[z_from(k)]
        for g in range(1, G):
            ag_y.append(go(copy(src, src, agy_s.at[g, k], agy_r.at[g, k], col=y_peer(g))))
    for one in ag_y:
        one.wait_recv()

    base = pl.multiple_of(c * share // LANES * LANES, LANES)
    wide = ipfull[:, :, pl.ds(base, LANES)].reshape(rows, LANES)
    picked = wide[:, :share]
    for q in range(1, packs):
        picked = jnp.where(c % packs == q, wide[:, q * share : (q + 1) * share], picked)
    ip_ref[...] = picked

    def update(i):
        at = pl.ds(pl.multiple_of(i * tile, tile), tile)
        per = tile // chunk
        piece = ipfull[pl.ds(i * per, per)].reshape(tile, width)
        return dot_split((wthi[:, at], wtlo[:, at]), split(piece))

    if rows == tile:
        product_part = update(0)
    else:
        product_part = lax.fori_loop(0, rows // tile, lambda i, t: t + update(i), jnp.zeros((cols, width), F32))
    for a in range(R):
        ppbuf[a] = product_part[:, a * pwidth : (a + 1) * pwidth]

    order = list(range(1, X)) + [0]
    near = [
        go(copy(ppbuf.at[over(x_peer(k))], ppair.at[k], f1_s.at[k], f1_r.at[k], row=partner)) for k in order
    ]
    far = []
    for one, k in zip(near, order):
        one.wait_recv()
        total = ppbuf[x_peer(k)] + ppair[k]
        if k:
            pxsend[k] = total
            far.append(go(copy(pxsend.at[k], pxrecv.at[k], f2_s.at[k], f2_r.at[k], row=x_peer(k))))
    for one, k in zip(far, range(1, X)):
        one.wait_recv()
        total = total + pxrecv[k]
    pp_ref[...] = total
    for one in pending:
        one.wait_send()


def body(R, C, G, diag_block, panel_below, trail_inverse):
    X, Z = R // 2, C // G
    width = diag_block.shape[0]
    rows, cols = trail_inverse.shape
    share, pwidth, chunk = width // C, width // R, rows // C
    part = width * share // LANES // R
    dma = pltpu.SemaphoreType.DMA
    V = pltpu.VMEM
    vmem = pl.BlockSpec(memory_space=pltpu.VMEM)
    return pl.pallas_call(
        functools.partial(kernel, R, C, G),
        out_shape=(
            jax.ShapeDtypeStruct((rows, share), F32),
            jax.ShapeDtypeStruct((cols, pwidth), F32),
        ),
        in_specs=[vmem] * 3,
        out_specs=(vmem, vmem),
        scratch_shapes=[
            V((R, C, part, LANES), F32),
            V((R, cols, pwidth), F32),
            V((cols, width), F32),
            V((rows, cols), BF16),
            V((rows, cols), BF16),
            V((cols, rows), BF16),
            V((cols, rows), BF16),
            V((rows, width), F32),
            V((G - 1, Z, chunk, width), F32),
            V((Z, chunk, width), F32),
            V((Z, chunk, width), F32),
            V((width, width), F32),
            V((width, width), F32),
            V((width, width), F32),
            V((8, width), F32),
            V((C, chunk, width), F32),
            V((R, cols, pwidth), F32),
            V((X, cols, pwidth), F32),
            V((X, cols, pwidth), F32),
            V((X, cols, pwidth), F32),
            dma((C,)), dma((C,)), dma((X,)), dma((X,)), dma((X,)), dma((X,)),
            dma((X,)), dma((X,)), dma((X,)), dma((X,)),
            dma((G, Z)), dma((G, Z)), dma((Z,)), dma((Z,)),
            dma((Z,)), dma((Z,)), dma((G, Z)), dma((G, Z)),
            dma((X,)), dma((X,)), dma((X,)), dma((X,)),
        ],
        compiler_params=pltpu.CompilerParams(
            collective_id=0, has_side_effects=True, vmem_limit_bytes=60 * 1024 * 1024
        ),
    )(diag_block, panel_below, trail_inverse)


def solution(mesh):
    R, C = mesh.shape["row"], mesh.shape["col"]
    placed = (P(None, "col"), P("col", "row"), P("row", "col"))
    return jax.shard_map(
        functools.partial(body, R, C, R // 2),
        mesh=mesh,
        in_specs=placed,
        out_specs=(P("row", "col"), P("col", "row")),
        check_vma=False,
    )
```

```python
import functools

import jax
import jax.numpy as jnp
from jax import lax
from jax.experimental import pallas as pl
from jax.experimental.pallas import tpu as pltpu
from jax.sharding import PartitionSpec as P

F32 = jnp.float32
BF16 = jnp.bfloat16
MESH = pl.DeviceIdType.MESH
LANES = 128
SEED = 16


def split(value):
    high = value.astype(BF16)
    return high, (value - high.astype(F32)).astype(BF16)


def dot_split(left, right):
    lh, ll = left
    rh, rl = right
    return (
        jnp.dot(lh, rh, preferred_element_type=F32)
        + jnp.dot(lh, rl, preferred_element_type=F32)
        + jnp.dot(ll, rh, preferred_element_type=F32)
    )


def dot3(left, right):
    return dot_split(split(left), split(right))


def repeat(count, step):
    if count == 1:
        step(0)
    else:
        lax.fori_loop(0, count, lambda i, _: (step(i), 0)[1], 0)


def invert_seed_blocks(m_ref, x_ref, dinv_ref, l_ref, width):
    row = lax.broadcasted_iota(jnp.int32, (LANES, LANES), 0)
    col = lax.broadcasted_iota(jnp.int32, (LANES, LANES), 1)
    eye = row == col
    low = row > col
    eye_f = jnp.where(eye, 1.0, 0.0).astype(F32)
    blocks = width // LANES
    ms, ns, ps = [], [], []
    for b in range(blocks):
        at = slice(b * LANES, (b + 1) * LANES)
        block = l_ref[at, at]
        diagonal = jnp.where(eye, block, 0.0)
        dinv_ref[0:1, at] = 1.0 / jnp.sum(diagonal, axis=0, keepdims=True)
        scale = 1.0 / jnp.sum(diagonal, axis=1, keepdims=True)
        if b:
            m_ref[at, 0 : b * LANES] = l_ref[at, 0 : b * LANES] * scale
        m = jnp.where(low, block * scale, 0.0)
        n = jnp.where(row // SEED == col // SEED, -m, 0.0)
        ms.append(m)
        ns.append(n)
        ps.append(eye_f + n)
    size = 2
    while size < SEED:
        halves = [split(n) for n in ns]
        ns = [dot_split(h, h) for h in halves]
        ps = [p + dot3(p, n) for p, n in zip(ps, ns)]
        size *= 2
    size = SEED
    while size < LANES:
        off = jnp.logical_and((row // size) % 2 == 1, col // size == row // size - 1)
        pairs = [split(p) for p in ps]
        mid = [dot_split(split(jnp.where(off, m, 0.0)), q) for m, q in zip(ms, pairs)]
        ps = [p - dot_split(q, split(t)) for p, q, t in zip(ps, pairs, mid)]
        size *= 2
    x_ref[...] = jnp.zeros_like(x_ref)
    for b in range(blocks):
        at = slice(b * LANES, (b + 1) * LANES)
        x_ref[at, at] = ps[b]


def invert_double(m_ref, x_ref, width):
    size = LANES
    while size < width:
        for p in range(0, width, 2 * size):
            a, b = slice(p, p + size), slice(p + size, p + 2 * size)
            x_ref[b, a] = -dot3(x_ref[b, b], dot3(m_ref[b, a], x_ref[a, a]))
        size *= 2


def kernel(
    R, C, G,
    diag_ref, panel_ref, trail_ref, ip_ref, pp_ref,
    lbuf, pbuf, pfull, whi, wlo, wthi, wtlo, zpart, yrecv, zsend, zrecv,
    diag_t, lmat, mmat, xmat, dinv, ipfull, ppbuf, ppair, pxsend, pxrecv,
    d1_s, d1_r, d2_s, d2_r, d2f_s, d2f_r, p_s, p_r, pf_s, pf_r,
    y_s, y_r, z_s, z_r, ag_s, ag_r, agy_s, agy_r, f1_s, f1_r, f2_s, f2_r,
):
    r, c = lax.axis_index("row"), lax.axis_index("col")
    X, Z = R // 2, C // G
    x, core = r // 2, r % 2
    z, y = c // G, c % G
    partner = x * 2 + 1 - core
    width = lmat.shape[0]
    share = width // C
    rows, cols = trail_ref.shape
    pwidth = width // R
    cycle = min(512, cols)
    chunks = rows // cycle
    sub = cycle // C

    def active(group, j):
        return group * G <= r + R * j

    def part_of(j):
        return pl.ds(j * sub, sub)

    def x_peer(k):
        return lax.rem(x + k, X) * 2 + core

    def x_from(k):
        return lax.rem(x + X - k, X) * 2 + core

    def over(a):
        return a // 2 * 2 + 1 - a % 2

    def z_peer(k):
        return lax.rem(z + k, Z) * G + y

    def z_from(k):
        return lax.rem(z + Z - k, Z) * G + y

    def y_peer(k):
        return z * G + lax.rem(y + k, G)

    def copy(src, dst, s, d, **where):
        return pltpu.make_async_remote_copy(
            src_ref=src, dst_ref=dst, send_sem=s, recv_sem=d,
            device_id=where, device_id_type=MESH,
        )

    for k in range(C):
        ipfull[k] = jnp.zeros(ipfull.shape[1:], F32)
    barrier = pltpu.get_barrier_semaphore()
    for k in range(1, R):
        pl.semaphore_signal(barrier, inc=1, device_id={"row": lax.rem(r + k, R)}, device_id_type=MESH)
    for k in range(1, C):
        pl.semaphore_signal(barrier, inc=1, device_id={"col": lax.rem(c + k, C)}, device_id_type=MESH)

    packs = LANES // share
    tall = width // packs
    part = tall // R
    diag_t[...] = diag_ref[...].T
    for q in range(packs):
        lbuf[r, c, :, q * share : (q + 1) * share] = diag_t[pl.ds(q * tall + r * part, part), :]
    pl.semaphore_wait(barrier, R + C - 2)

    pending = []

    def go(one):
        one.start()
        pending.append(one)
        return one

    held = []

    def go_if(when, one):
        pl.when(when)(one.start)
        held.append((when, one))
        return one

    p_far = [go(copy(panel_ref, pbuf.at[r], p_s.at[k], p_r.at[k], row=x_peer(k))) for k in range(1, X)]
    p_near = go(copy(panel_ref, pbuf.at[r], p_s.at[0], p_r.at[0], row=partner))
    d1 = [
        go(copy(lbuf.at[r, c], lbuf.at[r, c], d1_s.at[k], d1_r.at[k], col=lax.rem(c + k, C)))
        for k in range(1, C)
    ]
    pbuf[r] = panel_ref[...]

    tile = min(512, rows)

    def form(i):
        at = pl.ds(pl.multiple_of(i * tile, tile), tile)
        lr = lax.broadcasted_iota(jnp.int32, (tile, cols), 0) + i * tile
        lc = lax.broadcasted_iota(jnp.int32, (tile, cols), 1)
        gr = (lr // cycle * R + r) * cycle + lr % cycle
        gc = (lc // cycle * C + c) * cycle + lc % cycle
        w = jnp.where(gr >= gc, trail_ref[at, :], 0.0) + jnp.where(gr == gc, 1.0, 0.0).astype(F32)
        hi, lo = split(w)
        whi[at, :] = hi
        wlo[at, :] = lo
        hi, lo = split(w.T)
        wthi[:, at] = hi
        wtlo[:, at] = lo

    repeat(rows // tile, form)

    p_fwd = []
    for k in range(1, X):
        p_far[k - 1].wait_recv()
        src = pbuf.at[x_from(k)]
        p_fwd.append(go(copy(src, src, pf_s.at[k], pf_r.at[k], row=partner)))
    p_near.wait_recv()
    for one in p_fwd:
        one.wait_recv()
    for a in range(R):
        pfull[:, a * pwidth : (a + 1) * pwidth] = pbuf[a]
    pair = split(pfull[...])

    def product(i):
        at = pl.ds(pl.multiple_of(i * tile, tile), tile)
        zpart[at, :] = dot_split((whi[at, :], wlo[at, :]), pair)

    repeat(rows // tile, product)

    def rows_of(owner, j):
        return pl.ds(pl.multiple_of(j * cycle + owner * sub, sub), sub)

    order = list(range(1, Z)) + [0]
    y_sends = {}
    for k in order:
        for j in range(chunks):
            for g in range(1, G):
                owner = lax.rem(z + k, Z) * G + lax.rem(y + g, G)
                y_sends[k, j, g] = go_if(
                    active(z, j),
                    copy(
                        zpart.at[rows_of(owner, j), :], yrecv.at[g - 1, k, part_of(j)],
                        y_s.at[g, k, j], y_r.at[g, k, j], col=y_peer(g),
                    ),
                )

    for one in d1:
        one.wait_recv()
    d2_far = [go(copy(lbuf.at[r], lbuf.at[r], d2_s.at[k], d2_r.at[k], row=x_peer(k))) for k in range(1, X)]
    d2_near = go(copy(lbuf.at[r], lbuf.at[r], d2_s.at[0], d2_r.at[0], row=partner))

    z_sends = []
    d2_fwd = []
    for step, k in enumerate(order):
        for j in range(chunks):
            @pl.when(active(z, j))
            def _(k=k, j=j):
                total = zpart[rows_of(z_peer(k), j), :]
                for g in range(1, G):
                    y_sends[k, j, g].wait_recv()
                    total = total + yrecv[g - 1, k, part_of(j)]
                zsend[k, part_of(j)] = total

            if k == 0:

                @pl.when(jnp.logical_not(active(z, j)))
                def _(j=j):
                    zsend[0, part_of(j)] = jnp.zeros((sub, width), F32)

            else:
                sent = copy(
                    zsend.at[k, part_of(j)], zrecv.at[k, part_of(j)], z_s.at[k, j], z_r.at[k, j], col=z_peer(k)
                )
                z_sends.append((k, j, go_if(active(z, j), sent)))
        if step == Z // 2:
            for j in range(1, X):
                d2_far[j - 1].wait_recv()
                src = lbuf.at[x_from(j)]
                d2_fwd.append(go(copy(src, src, d2f_s.at[j], d2f_r.at[j], row=partner)))

    d2_near.wait_recv()
    for one in d2_fwd:
        one.wait_recv()
    for q in range(packs):
        for a in range(R):
            at = slice(q * tall + a * part, q * tall + (a + 1) * part)
            for b in range(C):
                lmat[at, b * share : (b + 1) * share] = lbuf[a, b, :, q * share : (q + 1) * share]
    invert_seed_blocks(mmat, xmat, dinv, lmat, width)
    invert_double(mmat, xmat, width)

    for k, j, one in z_sends:

        @pl.when(active(z_from(k) // G, j))
        def _(k=k, j=j, one=one):
            one.wait_recv()
            zsend[0, part_of(j)] = zsend[0, part_of(j)] + zrecv[k, part_of(j)]

    total = zsend[0]
    ipfull[c] = -dot3(total, xmat[...]) * dinv[0:1, :]

    def pass_on(owner, j, to_group, s, d, col):
        base = pl.multiple_of(to_group * G * share // LANES * LANES, LANES)
        full = ipfull.at[owner, part_of(j)]
        lanes = ipfull.at[owner, part_of(j), pl.ds(base, LANES)]
        return copy(full, full, s, d, col=col), copy(lanes, lanes, s, d, col=col)

    def send_either(when, pair):
        go_if(when, pair[0])
        go_if(jnp.logical_not(when), pair[1])

    def wait_either(when, pair):
        pl.when(when)(pair[0].wait_recv)
        pl.when(jnp.logical_not(when))(pair[1].wait_recv)

    here = [active(z, j) for j in range(chunks)]
    ag_y = []
    for k in range(1, Z):
        for j in range(chunks):
            to = lax.rem(z + k, Z)
            send_either(active(to, j), pass_on(c, j, to, ag_s.at[k, j], ag_r.at[k, j], z_peer(k)))

    def to_y(owner, k, j):
        for g in range(1, G):
            pair = pass_on(owner, j, z, agy_s.at[g, k, j], agy_r.at[g, k, j], y_peer(g))
            send_either(here[j], pair)
            ag_y.append((here[j], pair))

    for j in range(chunks):
        to_y(c, 0, j)
    for k in range(1, Z):
        for j in range(chunks):
            wait_either(here[j], pass_on(z_from(k), j, z, ag_s.at[k, j], ag_r.at[k, j], z_peer(k)))
            to_y(z_from(k), k, j)
    for when, pair in ag_y:
        wait_either(when, pair)

    base = pl.multiple_of(c * share // LANES * LANES, LANES)
    product_part = None
    for j in range(chunks):
        at = slice(j * cycle, (j + 1) * cycle)
        wide = ipfull[:, part_of(j), pl.ds(base, LANES)].reshape(cycle, LANES)
        picked = wide[:, :share]
        for q in range(1, packs):
            picked = jnp.where(c % packs == q, wide[:, q * share : (q + 1) * share], picked)
        ip_ref[:, at] = picked.T
        piece = ipfull[:, part_of(j), :].reshape(cycle, width)
        term = dot_split((wthi[:, at], wtlo[:, at]), split(piece))
        product_part = term if product_part is None else product_part + term
    for a in range(R):
        ppbuf[a] = product_part[:, a * pwidth : (a + 1) * pwidth]

    order = list(range(1, X)) + [0]
    near = [
        go(copy(ppbuf.at[over(x_peer(k))], ppair.at[k], f1_s.at[k], f1_r.at[k], row=partner)) for k in order
    ]
    far = []
    for one, k in zip(near, order):
        one.wait_recv()
        total = ppbuf[x_peer(k)] + ppair[k]
        if k:
            pxsend[k] = total
            far.append(go(copy(pxsend.at[k], pxrecv.at[k], f2_s.at[k], f2_r.at[k], row=x_peer(k))))
    for one, k in zip(far, range(1, X)):
        one.wait_recv()
        total = total + pxrecv[k]
    pp_ref[...] = total
    for one in pending:
        one.wait_send()
    for when, one in held:
        pl.when(when)(one.wait_send)


def body(R, C, G, diag_block, panel_below, trail_inverse):
    X, Z = R // 2, C // G
    width = diag_block.shape[0]
    rows, cols = trail_inverse.shape
    share, pwidth, chunk = width // C, width // R, rows // C
    part = width * share // LANES // R
    chunks = rows // min(512, cols)
    dma = pltpu.SemaphoreType.DMA
    V = pltpu.VMEM
    vmem = pl.BlockSpec(memory_space=pltpu.VMEM)
    inverse_t, product_panel = pl.pallas_call(
        functools.partial(kernel, R, C, G),
        out_shape=(
            jax.ShapeDtypeStruct((share, rows), F32),
            jax.ShapeDtypeStruct((cols, pwidth), F32),
        ),
        in_specs=[vmem] * 3,
        out_specs=(vmem, vmem),
        scratch_shapes=[
            V((R, C, part, LANES), F32),
            V((R, cols, pwidth), F32),
            V((cols, width), F32),
            V((rows, cols), BF16),
            V((rows, cols), BF16),
            V((cols, rows), BF16),
            V((cols, rows), BF16),
            V((rows, width), F32),
            V((G - 1, Z, chunk, width), F32),
            V((Z, chunk, width), F32),
            V((Z, chunk, width), F32),
            V((width, share), F32),
            V((width, width), F32),
            V((width, width), F32),
            V((width, width), F32),
            V((8, width), F32),
            V((C, chunk, width), F32),
            V((R, cols, pwidth), F32),
            V((X, cols, pwidth), F32),
            V((X, cols, pwidth), F32),
            V((X, cols, pwidth), F32),
            dma((C,)), dma((C,)), dma((X,)), dma((X,)), dma((X,)), dma((X,)),
            dma((X,)), dma((X,)), dma((X,)), dma((X,)),
            dma((G, Z, chunks)), dma((G, Z, chunks)), dma((Z, chunks)), dma((Z, chunks)),
            dma((Z, chunks)), dma((Z, chunks)), dma((G, Z, chunks)), dma((G, Z, chunks)),
            dma((X,)), dma((X,)), dma((X,)), dma((X,)),
        ],
        compiler_params=pltpu.CompilerParams(
            collective_id=0, has_side_effects=True, vmem_limit_bytes=60 * 1024 * 1024
        ),
    )(diag_block.T, panel_below, trail_inverse)
    return inverse_t.T, product_panel


def solution(mesh):
    R, C = mesh.shape["row"], mesh.shape["col"]
    placed = (P(None, "col"), P("col", "row"), P("row", "col"))
    return jax.shard_map(
        functools.partial(body, R, C, R // 2),
        mesh=mesh,
        in_specs=placed,
        out_specs=(P("row", "col"), P("col", "row")),
        check_vma=False,
    )
```

```python
import functools

import jax
import jax.numpy as jnp
from jax import lax
from jax.experimental import pallas as pl
from jax.experimental.pallas import tpu as pltpu
from jax.sharding import PartitionSpec as P

F32 = jnp.float32
BF16 = jnp.bfloat16
MESH = pl.DeviceIdType.MESH
LANES = 128
SEED = 16


def split(value):
    high = value.astype(BF16)
    return high, (value - high.astype(F32)).astype(BF16)


def dot_split(left, right):
    lh, ll = left
    rh, rl = right
    return (
        jnp.dot(lh, rh, preferred_element_type=F32)
        + jnp.dot(lh, rl, preferred_element_type=F32)
        + jnp.dot(ll, rh, preferred_element_type=F32)
    )


def dot3(left, right):
    return dot_split(split(left), split(right))


def repeat(count, step):
    if count == 1:
        step(0)
    else:
        lax.fori_loop(0, count, lambda i, _: (step(i), 0)[1], 0)


def invert_seed_blocks(m_ref, x_ref, dinv_ref, l_ref, width):
    row = lax.broadcasted_iota(jnp.int32, (LANES, LANES), 0)
    col = lax.broadcasted_iota(jnp.int32, (LANES, LANES), 1)
    eye = row == col
    low = row > col
    eye_f = jnp.where(eye, 1.0, 0.0).astype(F32)
    blocks = width // LANES
    ms, ns, ps = [], [], []
    for b in range(blocks):
        at = slice(b * LANES, (b + 1) * LANES)
        block = l_ref[at, at]
        diagonal = jnp.where(eye, block, 0.0)
        dinv_ref[0:1, at] = 1.0 / jnp.sum(diagonal, axis=0, keepdims=True)
        scale = 1.0 / jnp.sum(diagonal, axis=1, keepdims=True)
        if b:
            m_ref[at, 0 : b * LANES] = l_ref[at, 0 : b * LANES] * scale
        m = jnp.where(low, block * scale, 0.0)
        n = jnp.where(row // SEED == col // SEED, -m, 0.0)
        ms.append(m)
        ns.append(n)
        ps.append(eye_f + n)
    size = 2
    while size < SEED:
        halves = [split(n) for n in ns]
        ns = [dot_split(h, h) for h in halves]
        ps = [p + dot3(p, n) for p, n in zip(ps, ns)]
        size *= 2
    size = SEED
    while size < LANES:
        off = jnp.logical_and((row // size) % 2 == 1, col // size == row // size - 1)
        pairs = [split(p) for p in ps]
        mid = [dot_split(split(jnp.where(off, m, 0.0)), q) for m, q in zip(ms, pairs)]
        ps = [p - dot_split(q, split(t)) for p, q, t in zip(ps, pairs, mid)]
        size *= 2
    x_ref[...] = jnp.zeros_like(x_ref)
    for b in range(blocks):
        at = slice(b * LANES, (b + 1) * LANES)
        x_ref[at, at] = ps[b]


def invert_double(m_ref, x_ref, width):
    size = LANES
    while size < width:
        for p in range(0, width, 2 * size):
            a, b = slice(p, p + size), slice(p + size, p + 2 * size)
            x_ref[b, a] = -dot3(x_ref[b, b], dot3(m_ref[b, a], x_ref[a, a]))
        size *= 2


def kernel(
    R, C, G,
    diag_ref, panel_ref, trail_ref, ip_ref, pp_ref,
    lbuf, pbuf, pfull, whi, wlo, wthi, wtlo, zpart, yrecv, zsend, zrecv,
    diag_t, lmat, mmat, xmat, dinv, ipfull, ppbuf, ppair, pxsend, pxrecv,
    d1_s, d1_r, d2_s, d2_r, d2f_s, d2f_r, p_s, p_r, pf_s, pf_r,
    y_s, y_r, z_s, z_r, ag_s, ag_r, agy_s, agy_r, f1_s, f1_r, f2_s, f2_r,
):
    r, c = lax.axis_index("row"), lax.axis_index("col")
    X, Z = R // 2, C // G
    x, core = r // 2, r % 2
    z, y = c // G, c % G
    partner = x * 2 + 1 - core
    width = lmat.shape[0]
    share = width // C
    rows, cols = trail_ref.shape
    pwidth = width // R
    cycle = min(512, cols)
    chunks = rows // cycle
    sub = cycle // C

    def active(group, j):
        return group * G <= r + R * j

    def part_of(j):
        return pl.ds(j * sub, sub)

    def x_peer(k):
        return lax.rem(x + k, X) * 2 + core

    def x_from(k):
        return lax.rem(x + X - k, X) * 2 + core

    def over(a):
        return a // 2 * 2 + 1 - a % 2

    def z_peer(k):
        return lax.rem(z + k, Z) * G + y

    def z_from(k):
        return lax.rem(z + Z - k, Z) * G + y

    def y_peer(k):
        return z * G + lax.rem(y + k, G)

    def copy(src, dst, s, d, **where):
        return pltpu.make_async_remote_copy(
            src_ref=src, dst_ref=dst, send_sem=s, recv_sem=d,
            device_id=where, device_id_type=MESH,
        )

    for k in range(C):
        ipfull[k] = jnp.zeros(ipfull.shape[1:], F32)
    barrier = pltpu.get_barrier_semaphore()
    for k in range(1, R):
        pl.semaphore_signal(barrier, inc=1, device_id={"row": lax.rem(r + k, R)}, device_id_type=MESH)
    for k in range(1, C):
        pl.semaphore_signal(barrier, inc=1, device_id={"col": lax.rem(c + k, C)}, device_id_type=MESH)

    packs = LANES // share
    tall = width // packs
    part = tall // R
    diag_t[...] = diag_ref[...].T
    for q in range(packs):
        lbuf[r, c, :, q * share : (q + 1) * share] = diag_t[pl.ds(q * tall + r * part, part), :]
    pl.semaphore_wait(barrier, R + C - 2)

    pending = []

    def go(one):
        one.start()
        pending.append(one)
        return one

    held = []

    def go_if(when, one):
        pl.when(when)(one.start)
        held.append((when, one))
        return one

    p_far = [go(copy(panel_ref, pbuf.at[r], p_s.at[k], p_r.at[k], row=x_peer(k))) for k in range(1, X)]
    p_near = go(copy(panel_ref, pbuf.at[r], p_s.at[0], p_r.at[0], row=partner))
    d1 = [
        go(copy(lbuf.at[r, c], lbuf.at[r, c], d1_s.at[k], d1_r.at[k], col=lax.rem(c + k, C)))
        for k in range(1, C)
    ]
    pbuf[r] = panel_ref[...]

    tile = min(512, rows)

    def form(i):
        at = pl.ds(pl.multiple_of(i * tile, tile), tile)
        lr = lax.broadcasted_iota(jnp.int32, (tile, cols), 0) + i * tile
        lc = lax.broadcasted_iota(jnp.int32, (tile, cols), 1)
        gr = (lr // cycle * R + r) * cycle + lr % cycle
        gc = (lc // cycle * C + c) * cycle + lc % cycle
        w = jnp.where(gr >= gc, trail_ref[at, :], 0.0) + jnp.where(gr == gc, 1.0, 0.0).astype(F32)
        hi, lo = split(w)
        whi[at, :] = hi
        wlo[at, :] = lo
        hi, lo = split(w.T)
        wthi[:, at] = hi
        wtlo[:, at] = lo

    repeat(rows // tile, form)

    p_fwd = []
    for k in range(1, X):
        p_far[k - 1].wait_recv()
        src = pbuf.at[x_from(k)]
        p_fwd.append(go(copy(src, src, pf_s.at[k], pf_r.at[k], row=partner)))
    p_near.wait_recv()
    for one in p_fwd:
        one.wait_recv()
    for a in range(R):
        pfull[:, a * pwidth : (a + 1) * pwidth] = pbuf[a]
    pair = split(pfull[...])

    def product(i):
        at = pl.ds(pl.multiple_of(i * tile, tile), tile)
        zpart[at, :] = dot_split((whi[at, :], wlo[at, :]), pair)

    repeat(rows // tile, product)

    def rows_of(owner, j):
        return pl.ds(pl.multiple_of(j * cycle + owner * sub, sub), sub)

    order = list(range(1, Z)) + [0]
    y_sends = {}
    for k in order:
        for j in range(chunks):
            for g in range(1, G):
                owner = lax.rem(z + k, Z) * G + lax.rem(y + g, G)
                y_sends[k, j, g] = go_if(
                    active(z, j),
                    copy(
                        zpart.at[rows_of(owner, j), :], yrecv.at[g - 1, k, part_of(j)],
                        y_s.at[g, k, j], y_r.at[g, k, j], col=y_peer(g),
                    ),
                )

    for one in d1:
        one.wait_recv()
    d2_far = [go(copy(lbuf.at[r], lbuf.at[r], d2_s.at[k], d2_r.at[k], row=x_peer(k))) for k in range(1, X)]
    d2_near = go(copy(lbuf.at[r], lbuf.at[r], d2_s.at[0], d2_r.at[0], row=partner))

    z_sends = []
    d2_fwd = []
    for step, k in enumerate(order):
        for j in range(chunks):
            @pl.when(active(z, j))
            def _(k=k, j=j):
                total = zpart[rows_of(z_peer(k), j), :]
                for g in range(1, G):
                    y_sends[k, j, g].wait_recv()
                    total = total + yrecv[g - 1, k, part_of(j)]
                zsend[k, part_of(j)] = total

            if k == 0:

                @pl.when(jnp.logical_not(active(z, j)))
                def _(j=j):
                    zsend[0, part_of(j)] = jnp.zeros((sub, width), F32)

            else:
                sent = copy(
                    zsend.at[k, part_of(j)], zrecv.at[k, part_of(j)], z_s.at[k, j], z_r.at[k, j], col=z_peer(k)
                )
                z_sends.append((k, j, go_if(active(z, j), sent)))
        if step == Z // 2:
            for j in range(1, X):
                d2_far[j - 1].wait_recv()
                src = lbuf.at[x_from(j)]
                d2_fwd.append(go(copy(src, src, d2f_s.at[j], d2f_r.at[j], row=partner)))

    d2_near.wait_recv()
    for one in d2_fwd:
        one.wait_recv()
    for q in range(packs):
        for a in range(R):
            at = slice(q * tall + a * part, q * tall + (a + 1) * part)
            for b in range(C):
                lmat[at, b * share : (b + 1) * share] = lbuf[a, b, :, q * share : (q + 1) * share]
    invert_seed_blocks(mmat, xmat, dinv, lmat, width)
    invert_double(mmat, xmat, width)

    for k, j, one in z_sends:

        @pl.when(active(z_from(k) // G, j))
        def _(k=k, j=j, one=one):
            one.wait_recv()
            zsend[0, part_of(j)] = zsend[0, part_of(j)] + zrecv[k, part_of(j)]

    total = zsend[0]
    ipfull[c] = -dot3(total, xmat[...]) * dinv[0:1, :]

    def pass_on(owner, j, to_group, s, d, col):
        base = pl.multiple_of(to_group * G * share // LANES * LANES, LANES)
        full = ipfull.at[owner, part_of(j)]
        lanes = ipfull.at[owner, part_of(j), pl.ds(base, LANES)]
        return copy(full, full, s, d, col=col), copy(lanes, lanes, s, d, col=col)

    def send_either(when, pair):
        go_if(when, pair[0])
        go_if(jnp.logical_not(when), pair[1])

    def wait_either(when, pair):
        pl.when(when)(pair[0].wait_recv)
        pl.when(jnp.logical_not(when))(pair[1].wait_recv)

    here = [active(z, j) for j in range(chunks)]
    ag_y = []
    for k in range(1, Z):
        for j in range(chunks):
            to = lax.rem(z + k, Z)
            send_either(active(to, j), pass_on(c, j, to, ag_s.at[k, j], ag_r.at[k, j], z_peer(k)))

    def to_y(owner, k, j):
        for g in range(1, G):
            pair = pass_on(owner, j, z, agy_s.at[g, k, j], agy_r.at[g, k, j], y_peer(g))
            send_either(here[j], pair)
            ag_y.append((here[j], pair))

    for j in range(chunks):
        to_y(c, 0, j)
    for k in range(1, Z):
        for j in range(chunks):
            wait_either(here[j], pass_on(z_from(k), j, z, ag_s.at[k, j], ag_r.at[k, j], z_peer(k)))
            to_y(z_from(k), k, j)
    for when, pair in ag_y:
        wait_either(when, pair)

    order = list(range(1, X)) + [0]
    near = []
    for k in order:
        to = lax.rem(x + k, X)
        lanes = pl.ds(pl.multiple_of(to * 2 * pwidth, 2 * pwidth), 2 * pwidth)
        sums = None
        for j in range(chunks):
            at = slice(j * cycle, (j + 1) * cycle)
            piece = ipfull[:, part_of(j), lanes].reshape(cycle, 2 * pwidth)
            term = dot_split((wthi[:, at], wtlo[:, at]), split(piece))
            sums = term if sums is None else sums + term
        ppbuf[2 * to] = sums[:, :pwidth]
        ppbuf[2 * to + 1] = sums[:, pwidth:]
        near.append(go(copy(ppbuf.at[over(x_peer(k))], ppair.at[k], f1_s.at[k], f1_r.at[k], row=partner)))

    far = []
    for one, k in zip(near, order):
        one.wait_recv()
        total = ppbuf[x_peer(k)] + ppair[k]
        if k:
            pxsend[k] = total
            far.append(go(copy(pxsend.at[k], pxrecv.at[k], f2_s.at[k], f2_r.at[k], row=x_peer(k))))
    base = pl.multiple_of(c * share // LANES * LANES, LANES)
    for j in range(chunks):
        at = slice(j * cycle, (j + 1) * cycle)
        wide = ipfull[:, part_of(j), pl.ds(base, LANES)].reshape(cycle, LANES)
        picked = wide[:, :share]
        for q in range(1, packs):
            picked = jnp.where(c % packs == q, wide[:, q * share : (q + 1) * share], picked)
        ip_ref[:, at] = picked.T
    for one, k in zip(far, range(1, X)):
        one.wait_recv()
        total = total + pxrecv[k]
    pp_ref[...] = total
    for one in pending:
        one.wait_send()
    for when, one in held:
        pl.when(when)(one.wait_send)


def body(R, C, G, diag_block, panel_below, trail_inverse):
    X, Z = R // 2, C // G
    width = diag_block.shape[0]
    rows, cols = trail_inverse.shape
    share, pwidth, chunk = width // C, width // R, rows // C
    part = width * share // LANES // R
    chunks = rows // min(512, cols)
    dma = pltpu.SemaphoreType.DMA
    V = pltpu.VMEM
    vmem = pl.BlockSpec(memory_space=pltpu.VMEM)
    inverse_t, product_panel = pl.pallas_call(
        functools.partial(kernel, R, C, G),
        out_shape=(
            jax.ShapeDtypeStruct((share, rows), F32),
            jax.ShapeDtypeStruct((cols, pwidth), F32),
        ),
        in_specs=[vmem] * 3,
        out_specs=(vmem, vmem),
        scratch_shapes=[
            V((R, C, part, LANES), F32),
            V((R, cols, pwidth), F32),
            V((cols, width), F32),
            V((rows, cols), BF16),
            V((rows, cols), BF16),
            V((cols, rows), BF16),
            V((cols, rows), BF16),
            V((rows, width), F32),
            V((G - 1, Z, chunk, width), F32),
            V((Z, chunk, width), F32),
            V((Z, chunk, width), F32),
            V((width, share), F32),
            V((width, width), F32),
            V((width, width), F32),
            V((width, width), F32),
            V((8, width), F32),
            V((C, chunk, width), F32),
            V((R, cols, pwidth), F32),
            V((X, cols, pwidth), F32),
            V((X, cols, pwidth), F32),
            V((X, cols, pwidth), F32),
            dma((C,)), dma((C,)), dma((X,)), dma((X,)), dma((X,)), dma((X,)),
            dma((X,)), dma((X,)), dma((X,)), dma((X,)),
            dma((G, Z, chunks)), dma((G, Z, chunks)), dma((Z, chunks)), dma((Z, chunks)),
            dma((Z, chunks)), dma((Z, chunks)), dma((G, Z, chunks)), dma((G, Z, chunks)),
            dma((X,)), dma((X,)), dma((X,)), dma((X,)),
        ],
        compiler_params=pltpu.CompilerParams(
            collective_id=0, has_side_effects=True, vmem_limit_bytes=60 * 1024 * 1024
        ),
    )(diag_block.T, panel_below, trail_inverse)
    return inverse_t.T, product_panel


def solution(mesh):
    R, C = mesh.shape["row"], mesh.shape["col"]
    placed = (P(None, "col"), P("col", "row"), P("row", "col"))
    return jax.shard_map(
        functools.partial(body, R, C, R // 2),
        mesh=mesh,
        in_specs=placed,
        out_specs=(P("row", "col"), P("col", "row")),
        check_vma=False,
    )
```
